32 devices in a mesh: row: 4 (over y, core), col: 8 (over z, x).
Axes of the slice: x: 2, y: 2, z: 4, core: 2. Of those that a mesh axis runs over, the one named last changes fastest.
Arguments:
- queries: bfloat16 [128, 128, 1024], P(('row', 'col')), may hold values from -6 to 6
- coarse_keys: bfloat16 [512, 1024], P('row'), may hold values from -6 to 6
- fine_keys: bfloat16 [4096, 1024], P('col'), may hold values from -6 to 6
- super_ids: int32 [128, 16], P(('row', 'col')), may hold values from 0 to 511, as said below
- picks: int32 [128, 64], P(('row', 'col')), may hold values from 0 to 127, as said below
Outputs:
- importance: float32 [128, 8, 512], P(('row', 'col'))
- selected: float32 [128, 512], P(('row', 'col'))
The draws below stay inside these ranges and needn't reach their ends.
Inputs may be any that keep to these rules, and one draw needn't show every extreme that they name: `super_ids`: within each aligned run of 4 query blocks (the query blocks of one device), at most 16 of the ids lie in any one aligned range of 64 superblocks, and some range holds exactly 16; in some aligned group of 8 consecutive runs, one range holds exactly 16 ids of every run. Ids may repeat. `picks`: the numbers of a row are distinct; pick p names fine block p % 8 of superblock super_ids[b, p // 8]. Within each aligned run of 4 query blocks, at most 64 of the named fine blocks lie in any one aligned range of 64 superblocks, and some range holds exactly 64.
All inputs are finite; a program needn't handle non-finite values.
Results may differ from the reference program's by a relative error of at most 0.0003.
Values may be sent and summed in bfloat16 or wider, within the bound.
A program may use at most 64 MiB of HBM per device.

```python
import math
import jax
import jax.numpy as jnp
from jax import lax

H = 8
D = 128
QTOK = 128
SBLK = 8
NSEL = 16
PICK = 64
SUP_DEV = 64
QB_DEV = 4
SUPERS = 512
QB = 128
N_ROW = 4
N_COL = 8


def summary_table(key, salt, count):
    inner = jax.random.fold_in(key, salt)
    values = jnp.clip(jax.random.normal(inner, (count, H * D), jnp.float32), -6.0, 6.0)
    return values.astype(jnp.bfloat16)


def draw_queries(key, part):
    inner = jax.random.fold_in(key, 11)
    values = jnp.clip(jax.random.normal(inner, (QB, QTOK, H * D), jnp.float32), -6.0, 6.0)
    return values.astype(jnp.bfloat16)


def draw_coarse_keys(key, part):
    return summary_table(key, 12, SUPERS)


def draw_fine_keys(key, part):
    return summary_table(key, 13, SUPERS * SBLK)


def draw_super_ids(key, part):
    devices_all = N_ROW * N_COL
    base_owner = jax.random.randint(jax.random.fold_in(key, 21), (N_ROW,), 0, N_COL)
    spread = jax.random.randint(jax.random.fold_in(key, 22), (N_ROW,), 1, N_COL)
    zero_row = jax.random.randint(jax.random.fold_in(key, 23), (), 0, N_ROW)
    spread = jnp.where(jnp.arange(N_ROW, dtype=jnp.int32) == zero_row, 0, spread)
    device_ids = jnp.arange(devices_all, dtype=jnp.int32)
    row_of = device_ids // N_COL
    col_of = device_ids % N_COL
    hot_owner = (base_owner[row_of] + col_of * spread[row_of]) % N_COL
    rotation = jax.random.randint(jax.random.fold_in(key, 24), (devices_all,), 0, 4)
    block_ids = jnp.arange(QB, dtype=jnp.int32)
    device_of = block_ids // QB_DEV
    quarter = block_ids % QB_DEV // (QB_DEV // 4)
    classes = (quarter + rotation[device_of]) % 4
    counts = jnp.where(classes > 0, (N_COL - 1 - classes) // 3 + 1, 1)
    member = jax.random.randint(jax.random.fold_in(key, 25), (QB, NSEL), 0, counts[:, None])
    offsets = jnp.where(classes[:, None] == 0, 0, classes[:, None] + 3 * member)
    owners = (hot_owner[device_of][:, None] + offsets) % N_COL
    local_ids = jax.random.randint(jax.random.fold_in(key, 26), (QB, NSEL), 0, SUP_DEV)
    return (owners * SUP_DEV + local_ids).astype(jnp.int32)


def draw_picks(key, part):
    candidates = NSEL * SBLK
    scores = jax.random.randint(jax.random.fold_in(key, 31), (QB, candidates), 0, 2 ** 20)
    scores = scores * candidates + jnp.arange(candidates, dtype=jnp.int32)[None, :]
    order = jnp.argsort(scores, axis=-1)
    return order[:, :PICK].astype(jnp.int32)


def setup_inputs(seed: int = 0) -> dict:
    streams_of = jax.random.split(jax.random.key(seed), 6)
    queries = draw_queries(jax.random.fold_in(streams_of[5], 71), 0)
    coarse_keys = draw_coarse_keys(jax.random.fold_in(streams_of[5], 71), 0)
    fine_keys = draw_fine_keys(jax.random.fold_in(streams_of[5], 71), 0)
    super_ids = draw_super_ids(jax.random.fold_in(streams_of[5], 71), 0)
    picks = draw_picks(jax.random.fold_in(streams_of[5], 71), 0)
    return dict(queries=queries, coarse_keys=coarse_keys, fine_keys=fine_keys, super_ids=super_ids, picks=picks)


def reference(queries, coarse_keys, fine_keys, super_ids, picks):
    factor = 1.0 / math.sqrt(D)
    qheads = queries.reshape(QB, QTOK, H, D)
    coarse_heads = coarse_keys.reshape(SUPERS, H, D).astype(jnp.float32)

    def coarse_block(query_block):
        scores = jnp.einsum('thd,chd->htc', query_block.astype(jnp.float32), coarse_heads) * factor
        softened = jax.nn.softmax(scores, axis=-1)
        return lax.optimization_barrier(jnp.sum(softened, axis=1)) * (SUPERS / QTOK)
    importance = lax.map(coarse_block, qheads)
    parents = jnp.take_along_axis(super_ids, (picks // SBLK).astype(jnp.int32), axis=1).astype(jnp.int32)
    fine_ids = (parents * SBLK + picks % SBLK).astype(jnp.int32)
    weights = jnp.take_along_axis(importance, jnp.broadcast_to(parents[:, None, :], (QB, H, PICK)), axis=2)

    def fine_block(inputs):
        query_block, block_ids, block_weights = inputs
        fetched = jnp.take(fine_keys, block_ids, axis=0).reshape(PICK, H, D).astype(jnp.float32)
        scores = jnp.einsum('thd,jhd->htj', query_block.astype(jnp.float32), fetched) * factor
        softened = jax.nn.softmax(scores, axis=-1)
        return (lax.optimization_barrier(jnp.sum(softened, axis=1)) * block_weights * (PICK / QTOK)).reshape(H * PICK)
    selected = lax.map(fine_block, (qheads, fine_ids, weights))
    return (importance, selected)
```

```python
import functools
import math

import jax
import jax.numpy as jnp
from jax import lax
from jax.experimental import pallas as pl
from jax.experimental.pallas import tpu as pltpu
from jax.sharding import PartitionSpec as P

H = 8
D = 128
SBLK = 8
PICK = 64
LANES = 128
GROUP = 4
MESH = pl.DeviceIdType.MESH


def pack_requests(owners, local_ids, ncols, capacity):
    count = owners.shape[0]
    order = jnp.arange(count, dtype=jnp.int32)
    earlier = (owners[:, None] == owners[None, :]) & (order[None, :] < order[:, None])
    slots = jnp.sum(earlier.astype(jnp.int32), axis=1)
    places = owners * capacity + slots
    cells = jnp.arange(ncols * capacity, dtype=jnp.int32)
    matches = places[:, None] == cells[None, :]
    outgoing = jnp.sum(jnp.where(matches, local_ids[:, None] + 1, 0), axis=0) - 1
    return (outgoing.reshape(ncols, capacity), places)


def kernel(
    nrows,
    ncols,
    capacity,
    request_ref,
    place_ref,
    parent_ref,
    query_hbm,
    coarse_hbm,
    fine_hbm,
    portion_ref,
    selected_ref,
    query,
    fine,
    coarse,
    asked,
    staged,
    replies,
    weights,
    local_sem,
    coarse_send,
    coarse_recv,
    ask_send,
    ask_recv,
    reply_send,
    reply_recv,
):
    row = lax.axis_index("row")
    col = lax.axis_index("col")
    blocks, qtok, width = query.shape
    supers = nrows * coarse.shape[1]
    span = fine.shape[0]
    scale = math.log2(math.e) / math.sqrt(D)

    fine_copy = pltpu.make_async_copy(fine_hbm, fine, local_sem.at[0])
    query_copy = pltpu.make_async_copy(query_hbm, query, local_sem.at[1])
    own_copy = pltpu.make_async_copy(coarse_hbm, coarse.at[row], local_sem.at[2])
    fine_copy.start()
    query_copy.start()
    own_copy.start()

    barrier = pltpu.get_barrier_semaphore()

    def greet_col(k, carry):
        peer = lax.rem(col + k, ncols)
        pl.semaphore_signal(barrier, inc=1, device_id=(row, peer), device_id_type=MESH)
        return carry

    def greet_row(k, carry):
        peer = lax.rem(row + k, nrows)
        pl.semaphore_signal(barrier, inc=1, device_id=(peer, col), device_id_type=MESH)
        return carry

    lax.fori_loop(1, ncols, greet_col, 0)
    lax.fori_loop(1, nrows, greet_row, 0)
    pl.semaphore_wait(barrier, ncols + nrows - 2)

    def ask_copy(k):
        peer = lax.rem(col + k, ncols)
        return pltpu.make_async_remote_copy(
            src_ref=request_ref.at[peer],
            dst_ref=asked.at[k],
            send_sem=ask_send.at[k],
            recv_sem=ask_recv.at[k],
            device_id=(row, peer),
            device_id_type=MESH,
        )

    def reply_copy(k):
        peer = lax.rem(col - k + ncols, ncols)
        return pltpu.make_async_remote_copy(
            src_ref=staged.at[k],
            dst_ref=replies.at[col],
            send_sem=reply_send.at[k],
            recv_sem=reply_recv.at[k],
            device_id=(row, peer),
            device_id_type=MESH,
        )

    def coarse_copy(k):
        peer = lax.rem(row + k, nrows)
        return pltpu.make_async_remote_copy(
            src_ref=coarse_hbm,
            dst_ref=coarse.at[row],
            send_sem=coarse_send.at[k],
            recv_sem=coarse_recv.at[k],
            device_id=(peer, col),
            device_id_type=MESH,
        )

    def each(start, stop, act):
        def body(k, carry):
            act(k)
            return carry

        lax.fori_loop(start, stop, body, 0)

    each(1, ncols, lambda k: ask_copy(k).start())
    each(1, nrows, lambda k: coarse_copy(k).start())

    fine_copy.wait()
    asked[0] = request_ref[col]
    row_iota = lax.broadcasted_iota(jnp.int32, (capacity, span), 1)

    def stage_group(g, carry):
        picked = []
        for i in range(GROUP):
            k = g * GROUP + i

            @pl.when(k > 0)
            def _():
                ask_copy(k).wait_recv()

            ids = jnp.transpose(asked[k])[:capacity, 0:1]
            picked.append((ids == row_iota).astype(jnp.float32).astype(jnp.bfloat16))
        found = jnp.dot(
            jnp.concatenate(picked, axis=0), fine[...], preferred_element_type=jnp.float32
        ).astype(jnp.bfloat16)
        for i in range(GROUP):
            staged[g * GROUP + i] = found[i * capacity : (i + 1) * capacity]
        for i in range(GROUP):
            k = g * GROUP + i

            @pl.when(k > 0)
            def _():
                reply_copy(k).start()

        return carry

    lax.fori_loop(0, ncols // GROUP, stage_group, 0)
    replies[col] = staged[0]

    query_copy.wait()
    own_copy.wait()
    each(1, nrows, lambda k: coarse_copy(k).wait_recv())

    super_iota = lax.broadcasted_iota(jnp.int32, (supers, LANES), 0)

    def coarse_block(b, carry):
        for h in range(H):
            cut = pl.ds(h * D, D)
            keys = coarse[:, :, cut].reshape(supers, D)
            scores = lax.dot_general(
                query[b, :, cut], keys, (((1,), (1,)), ((), ())), preferred_element_type=jnp.float32
            )
            top = jnp.max(scores, axis=1, keepdims=True)
            raised = jnp.exp2((scores - top) * scale)
            share = 1.0 / jnp.sum(raised, axis=1, keepdims=True)
            portion_ref[b, h : h + 1, :] = jnp.sum(raised * share, axis=0, keepdims=True) * (
                supers / qtok
            )
        chosen = (parent_ref[b] == super_iota).astype(jnp.float32)
        weights[b] = jnp.dot(
            portion_ref[b],
            chosen,
            preferred_element_type=jnp.float32,
            precision=lax.Precision.HIGHEST,
        )
        return carry

    lax.fori_loop(0, blocks, coarse_block, 0)

    each(1, ncols, lambda k: reply_copy(k).wait_recv())
    places = jnp.transpose(place_ref[...])
    cell_iota = lax.broadcasted_iota(jnp.int32, (PICK, ncols * capacity), 1)
    sorter = jnp.concatenate(
        [
            (places[:PICK, b : b + 1] == cell_iota).astype(jnp.float32).astype(jnp.bfloat16)
            for b in range(blocks)
        ],
        axis=0,
    )
    fetched = jnp.dot(
        sorter,
        replies[...].reshape(ncols * capacity, width),
        preferred_element_type=jnp.float32,
    ).astype(jnp.bfloat16)
    for b in range(blocks):
        sums = []
        for h in range(H):
            keys = fetched[b * PICK : (b + 1) * PICK, h * D : (h + 1) * D]
            scores = lax.dot_general(
                query[b, :, h * D : (h + 1) * D],
                keys,
                (((1,), (1,)), ((), ())),
                preferred_element_type=jnp.float32,
            )
            top = jnp.max(scores, axis=1, keepdims=True)
            raised = jnp.exp2((scores - top) * scale)
            share = 1.0 / jnp.sum(raised, axis=1, keepdims=True)
            sums.append(jnp.sum(raised * share, axis=0, keepdims=True))
        selected_ref[b] = (
            jnp.concatenate(sums, axis=0) * weights[b, :, :PICK] * (PICK / qtok)
        )

    each(1, ncols, lambda k: ask_copy(k).wait_send())
    each(1, ncols, lambda k: reply_copy(k).wait_send())
    each(1, nrows, lambda k: coarse_copy(k).wait_send())


def per_device(queries, coarse_keys, fine_keys, super_ids, picks):
    blocks, qtok, width = queries.shape
    nrows = lax.axis_size("row")
    ncols = lax.axis_size("col")
    shard = coarse_keys.shape[0]
    supers = shard * nrows
    span = fine_keys.shape[0]
    capacity = blocks // 4 * PICK
    candidate = picks // SBLK
    which = jnp.arange(super_ids.shape[1], dtype=jnp.int32)
    parents = jnp.sum(
        jnp.where(candidate[:, :, None] == which, super_ids[:, None, :], 0), axis=2
    )
    fine_ids = parents * SBLK + picks % SBLK
    owners = (fine_ids // span).reshape(-1)
    local_ids = (fine_ids % span).reshape(-1)
    outgoing, places = pack_requests(owners, local_ids, ncols, capacity)
    requests = jnp.broadcast_to(
        jnp.pad(outgoing, ((0, 0), (0, LANES - capacity)))[:, None, :], (ncols, 8, LANES)
    )
    placed = jnp.pad(places.reshape(blocks, PICK), ((0, 8 - blocks), (0, LANES - PICK)))
    parented = jnp.pad(parents, ((0, 0), (0, LANES - PICK)))[:, None, :]
    vmem = pl.BlockSpec(memory_space=pltpu.VMEM)
    anywhere = pl.BlockSpec(memory_space=pl.ANY)
    portion, selected = pl.pallas_call(
        functools.partial(kernel, nrows, ncols, capacity),
        out_shape=(
            jax.ShapeDtypeStruct((blocks, H, supers), jnp.float32),
            jax.ShapeDtypeStruct((blocks, H, PICK), jnp.float32),
        ),
        in_specs=[vmem] * 3 + [anywhere] * 3,
        out_specs=(vmem, vmem),
        scratch_shapes=[
            pltpu.VMEM((blocks, qtok, width), jnp.bfloat16),
            pltpu.VMEM((span, width), jnp.bfloat16),
            pltpu.VMEM((nrows, shard, width), jnp.bfloat16),
            pltpu.VMEM((ncols, 8, LANES), jnp.int32),
            pltpu.VMEM((ncols, capacity, width), jnp.bfloat16),
            pltpu.VMEM((ncols, capacity, width), jnp.bfloat16),
            pltpu.VMEM((blocks, H, LANES), jnp.float32),
            pltpu.SemaphoreType.DMA((3,)),
            pltpu.SemaphoreType.DMA((nrows,)),
            pltpu.SemaphoreType.DMA((nrows,)),
            pltpu.SemaphoreType.DMA((ncols,)),
            pltpu.SemaphoreType.DMA((ncols,)),
            pltpu.SemaphoreType.DMA((ncols,)),
            pltpu.SemaphoreType.DMA((ncols,)),
        ],
        compiler_params=pltpu.CompilerParams(
            collective_id=0, has_side_effects=True, vmem_limit_bytes=50 * 1024 * 1024
        ),
    )(requests, placed, parented, queries, coarse_keys, fine_keys)
    return (portion, selected.reshape(blocks, H * PICK))


def solution(mesh):
    return jax.shard_map(
        per_device,
        mesh=mesh,
        in_specs=(
            P(("row", "col"), None, None),
            P("row", None),
            P("col", None),
            P(("row", "col"), None),
            P(("row", "col"), None),
        ),
        out_specs=(P(("row", "col"), None, None), P(("row", "col"), None)),
        check_vma=False,
    )
```

```python
import functools
import math

import jax
import jax.numpy as jnp
from jax import lax
from jax.experimental import pallas as pl
from jax.experimental.pallas import tpu as pltpu
from jax.sharding import PartitionSpec as P

H = 8
D = 128
SBLK = 8
PICK = 64
LANES = 128
GROUP = 4
MESH = pl.DeviceIdType.MESH


def pack_requests(owners, local_ids, ncols, capacity):
    count = owners.shape[0]
    order = jnp.arange(count, dtype=jnp.int32)
    earlier = (owners[:, None] == owners[None, :]) & (order[None, :] < order[:, None])
    slots = jnp.sum(earlier.astype(jnp.int32), axis=1)
    places = owners * capacity + slots
    cells = jnp.arange(ncols * capacity, dtype=jnp.int32)
    matches = places[:, None] == cells[None, :]
    outgoing = jnp.sum(jnp.where(matches, local_ids[:, None] + 1, 0), axis=0) - 1
    return (outgoing.reshape(ncols, capacity), places)


def kernel(
    nrows,
    ncols,
    capacity,
    request_ref,
    place_ref,
    parent_ref,
    query_hbm,
    coarse_hbm,
    fine_hbm,
    portion_ref,
    selected_ref,
    query,
    fine,
    coarse,
    across,
    asked,
    near_staged,
    far_staged,
    near,
    far,
    weights,
    local_sem,
    across_sem,
    coarse_send,
    coarse_recv,
    ask_send,
    ask_recv,
    near_send,
    near_recv,
    far_send,
    far_recv,
):
    row = lax.axis_index("row")
    col = lax.axis_index("col")
    half = ncols // 2
    team = nrows * half
    local = lax.rem(col, half)
    base = col - local
    me = row * half + local
    blocks, qtok, width = query.shape
    part = width // nrows
    supers = nrows * coarse.shape[1]
    span = fine.shape[0]
    scale = math.log2(math.e) / math.sqrt(D)

    fine_copy = pltpu.make_async_copy(fine_hbm, fine, local_sem.at[0])
    query_copy = pltpu.make_async_copy(query_hbm, query, local_sem.at[1])
    own_copy = pltpu.make_async_copy(coarse_hbm, coarse.at[row], local_sem.at[2])
    fine_copy.start()
    own_copy.start()
    query_copy.start()

    def each(start, stop, act):
        def body(k, carry):
            act(k)
            return carry

        lax.fori_loop(start, stop, body, 0)

    def ahead(k):
        peer = lax.rem(me + k, team)
        return (peer // half, base + lax.rem(peer, half))

    def behind(k):
        peer = lax.rem(me - k + team, team)
        return (peer // half, base + lax.rem(peer, half))

    opposite = (row, lax.rem(col + half, ncols))
    barrier = pltpu.get_barrier_semaphore()
    pl.semaphore_signal(barrier, inc=1, device_id=opposite, device_id_type=MESH)
    each(
        1,
        team,
        lambda k: pl.semaphore_signal(barrier, inc=1, device_id=ahead(k), device_id_type=MESH),
    )
    pl.semaphore_wait(barrier, team)

    def ask_copy(k):
        target = ahead(k)
        return pltpu.make_async_remote_copy(
            src_ref=request_ref.at[target[1] - base],
            dst_ref=asked.at[k],
            send_sem=ask_send.at[k],
            recv_sem=ask_recv.at[k],
            device_id=target,
            device_id_type=MESH,
        )

    across_copy = pltpu.make_async_remote_copy(
        src_ref=fine_hbm.at[:, pl.ds(pl.multiple_of(row * part, part), part)],
        dst_ref=across,
        send_sem=across_sem.at[0],
        recv_sem=across_sem.at[1],
        device_id=opposite,
        device_id_type=MESH,
    )

    def near_copy(k):
        return pltpu.make_async_remote_copy(
            src_ref=near_staged.at[k],
            dst_ref=near.at[local],
            send_sem=near_send.at[k],
            recv_sem=near_recv.at[k],
            device_id=(row, base + lax.rem(local - k + half, half)),
            device_id_type=MESH,
        )

    def far_copy(k):
        return pltpu.make_async_remote_copy(
            src_ref=far_staged.at[k],
            dst_ref=far.at[row, local],
            send_sem=far_send.at[k],
            recv_sem=far_recv.at[k],
            device_id=behind(k),
            device_id_type=MESH,
        )

    def coarse_copy(k):
        return pltpu.make_async_remote_copy(
            src_ref=coarse_hbm,
            dst_ref=coarse.at[row],
            send_sem=coarse_send.at[k],
            recv_sem=coarse_recv.at[k],
            device_id=(lax.rem(row + k, nrows), col),
            device_id_type=MESH,
        )

    each(1, team, lambda k: ask_copy(k).start())
    across_copy.start()
    each(1, nrows, lambda k: coarse_copy(k).start())

    asked[0] = request_ref[local]
    row_iota = lax.broadcasted_iota(jnp.int32, (capacity, span), 1)
    fine_copy.wait()
    each(1, team, lambda k: ask_copy(k).wait_recv())

    def one_hot(k, offset):
        ids = jnp.transpose(asked[k])[offset : offset + capacity, 0:1]
        return (ids == row_iota).astype(jnp.float32).astype(jnp.bfloat16)

    def near_group(g, carry):
        picked = []
        for i in range(GROUP):
            other = lax.rem(local - (g * GROUP + i) + half, half)
            picked.append(one_hot(lax.rem(local - other + team, team), 0))
        found = jnp.dot(
            jnp.concatenate(picked, axis=0), fine[...], preferred_element_type=jnp.float32
        ).astype(jnp.bfloat16)
        for i in range(GROUP):
            near_staged[g * GROUP + i] = found[i * capacity : (i + 1) * capacity]
        for i in range(GROUP):
            k = g * GROUP + i

            @pl.when(k > 0)
            def _():
                near_copy(k).start()

        return carry

    lax.fori_loop(0, half // GROUP, near_group, 0)
    near[local] = near_staged[0]
    across_copy.wait_recv()

    def far_group(g, carry):
        picked = [one_hot(g * GROUP + i, capacity) for i in range(GROUP)]
        found = jnp.dot(
            jnp.concatenate(picked, axis=0), across[...], preferred_element_type=jnp.float32
        ).astype(jnp.bfloat16)
        for i in range(GROUP):
            far_staged[g * GROUP + i] = found[i * capacity : (i + 1) * capacity]
        for i in range(GROUP):
            k = g * GROUP + i

            @pl.when(k > 0)
            def _():
                far_copy(k).start()

        return carry

    lax.fori_loop(0, team // GROUP, far_group, 0)
    far[row, local] = far_staged[0]

    query_copy.wait()
    own_copy.wait()
    each(1, nrows, lambda k: coarse_copy(k).wait_recv())

    super_iota = lax.broadcasted_iota(jnp.int32, (supers, LANES), 0)

    def coarse_block(b, carry):
        for h in range(H):
            cut = pl.ds(h * D, D)
            keys = coarse[:, :, cut].reshape(supers, D)
            scores = lax.dot_general(
                query[b, :, cut], keys, (((1,), (1,)), ((), ())), preferred_element_type=jnp.float32
            )
            top = jnp.max(scores, axis=1, keepdims=True)
            raised = jnp.exp2((scores - top) * scale)
            share = 1.0 / jnp.sum(raised, axis=1, keepdims=True)
            portion_ref[b, h : h + 1, :] = jnp.sum(raised * share, axis=0, keepdims=True) * (
                supers / qtok
            )
        chosen = (parent_ref[b] == super_iota).astype(jnp.float32)
        weights[b] = jnp.dot(
            portion_ref[b],
            chosen,
            preferred_element_type=jnp.float32,
            precision=lax.Precision.HIGHEST,
        )
        return carry

    lax.fori_loop(0, blocks, coarse_block, 0)

    places = jnp.transpose(place_ref[...])
    cell_iota = lax.broadcasted_iota(jnp.int32, (PICK, ncols * capacity), 1)
    sorter = jnp.concatenate(
        [
            (places[:PICK, b : b + 1] == cell_iota).astype(jnp.float32).astype(jnp.bfloat16)
            for b in range(blocks)
        ],
        axis=0,
    )
    cells = half * capacity
    each(1, half, lambda k: near_copy(k).wait_recv())
    each(1, team, lambda k: far_copy(k).wait_recv())
    sums = [[] for _ in range(blocks)]
    for q in range(nrows):
        rows = jnp.dot(
            sorter[:, :cells],
            near[:, :, q * part : (q + 1) * part].reshape(cells, part),
            preferred_element_type=jnp.float32,
        ) + jnp.dot(
            sorter[:, cells:],
            far[q].reshape(cells, part),
            preferred_element_type=jnp.float32,
        )
        rows = rows.astype(jnp.bfloat16)
        for b in range(blocks):
            for i in range(part // D):
                h = q * (part // D) + i
                scores = lax.dot_general(
                    query[b, :, h * D : (h + 1) * D],
                    rows[b * PICK : (b + 1) * PICK, i * D : (i + 1) * D],
                    (((1,), (1,)), ((), ())),
                    preferred_element_type=jnp.float32,
                )
                top = jnp.max(scores, axis=1, keepdims=True)
                raised = jnp.exp2((scores - top) * scale)
                share = 1.0 / jnp.sum(raised, axis=1, keepdims=True)
                sums[b].append(jnp.sum(raised * share, axis=0, keepdims=True))
    for b in range(blocks):
        selected_ref[b] = (
            jnp.concatenate(sums[b], axis=0) * weights[b, :, :PICK] * (PICK / qtok)
        )

    across_copy.wait_send()
    each(1, team, lambda k: ask_copy(k).wait_send())
    each(1, half, lambda k: near_copy(k).wait_send())
    each(1, team, lambda k: far_copy(k).wait_send())
    each(1, nrows, lambda k: coarse_copy(k).wait_send())


def per_device(queries, coarse_keys, fine_keys, super_ids, picks):
    blocks, qtok, width = queries.shape
    nrows = lax.axis_size("row")
    ncols = lax.axis_size("col")
    half = ncols // 2
    team = nrows * half
    shard = coarse_keys.shape[0]
    supers = shard * nrows
    span = fine_keys.shape[0]
    part = width // nrows
    capacity = blocks // 4 * PICK
    candidate = picks // SBLK
    which = jnp.arange(super_ids.shape[1], dtype=jnp.int32)
    parents = jnp.sum(
        jnp.where(candidate[:, :, None] == which, super_ids[:, None, :], 0), axis=2
    )
    fine_ids = parents * SBLK + picks % SBLK
    base = lax.axis_index("col") // half * half
    owners = ((fine_ids // span - base + ncols) % ncols).reshape(-1)
    local_ids = (fine_ids % span).reshape(-1)
    outgoing, places = pack_requests(owners, local_ids, ncols, capacity)
    outgoing = jnp.concatenate([outgoing[:half], outgoing[half:]], axis=1)
    requests = jnp.broadcast_to(outgoing[:, None, :], (half, 8, 2 * capacity))
    placed = jnp.pad(places.reshape(blocks, PICK), ((0, 8 - blocks), (0, LANES - PICK)))
    parented = jnp.pad(parents, ((0, 0), (0, LANES - PICK)))[:, None, :]
    vmem = pl.BlockSpec(memory_space=pltpu.VMEM)
    anywhere = pl.BlockSpec(memory_space=pl.ANY)
    dma = pltpu.SemaphoreType.DMA
    portion, selected = pl.pallas_call(
        functools.partial(kernel, nrows, ncols, capacity),
        out_shape=(
            jax.ShapeDtypeStruct((blocks, H, supers), jnp.float32),
            jax.ShapeDtypeStruct((blocks, H, PICK), jnp.float32),
        ),
        in_specs=[vmem] * 3 + [anywhere] * 3,
        out_specs=(vmem, vmem),
        scratch_shapes=[
            pltpu.VMEM((blocks, qtok, width), jnp.bfloat16),
            pltpu.VMEM((span, width), jnp.bfloat16),
            pltpu.VMEM((nrows, shard, width), jnp.bfloat16),
            pltpu.VMEM((span, part), jnp.bfloat16),
            pltpu.VMEM((team, 8, 2 * capacity), jnp.int32),
            pltpu.VMEM((half, capacity, width), jnp.bfloat16),
            pltpu.VMEM((team, capacity, part), jnp.bfloat16),
            pltpu.VMEM((half, capacity, width), jnp.bfloat16),
            pltpu.VMEM((nrows, half, capacity, part), jnp.bfloat16),
            pltpu.VMEM((blocks, H, LANES), jnp.float32),
            dma((3,)),
            dma((2,)),
            dma((nrows,)),
            dma((nrows,)),
            dma((team,)),
            dma((team,)),
            dma((half,)),
            dma((half,)),
            dma((team,)),
            dma((team,)),
        ],
        compiler_params=pltpu.CompilerParams(
            collective_id=0, has_side_effects=True, vmem_limit_bytes=50 * 1024 * 1024
        ),
    )(requests, placed, parented, queries, coarse_keys, fine_keys)
    return (portion, selected.reshape(blocks, H * PICK))


def solution(mesh):
    return jax.shard_map(
        per_device,
        mesh=mesh,
        in_specs=(
            P(("row", "col"), None, None),
            P("row", None),
            P("col", None),
            P(("row", "col"), None),
            P(("row", "col"), None),
        ),
        out_specs=(P(("row", "col"), None, None), P(("row", "col"), None)),
        check_vma=False,
    )
```

```python
import functools
import math

import jax
import jax.numpy as jnp
from jax import lax
from jax.experimental import pallas as pl
from jax.experimental.pallas import tpu as pltpu
from jax.sharding import PartitionSpec as P

H = 8
D = 128
SBLK = 8
PICK = 64
LANES = 128
GROUP = 4
MESH = pl.DeviceIdType.MESH


def log2(value):
    assert value & (value - 1) == 0
    return value.bit_length() - 1


def kernel(
    nrows,
    ncols,
    capacity,
    super_hbm,
    pick_hbm,
    query_hbm,
    coarse_hbm,
    fine_hbm,
    portion_ref,
    selected_ref,
    query,
    fine,
    coarse,
    across,
    asked,
    near_staged,
    far_staged,
    near,
    far,
    weights,
    chosen_ids,
    picked_ids,
    table,
    request,
    sorter,
    local_sem,
    across_sem,
    coarse_send,
    coarse_recv,
    ask_send,
    ask_recv,
    near_send,
    near_recv,
    far_send,
    far_recv,
):
    row = lax.axis_index("row")
    col = lax.axis_index("col")
    half = ncols // 2
    team = nrows * half
    local = lax.rem(col, half)
    base = col - local
    me = row * half + local
    blocks, qtok, width = query.shape
    part = width // nrows
    supers = nrows * coarse.shape[1]
    span = fine.shape[0]
    scale = math.log2(math.e) / math.sqrt(D)

    super_copy = pltpu.make_async_copy(super_hbm, chosen_ids, local_sem.at[3])
    pick_copy = pltpu.make_async_copy(pick_hbm, picked_ids, local_sem.at[4])
    super_copy.start()
    pick_copy.start()
    fine_copy = pltpu.make_async_copy(fine_hbm, fine, local_sem.at[0])
    query_copy = pltpu.make_async_copy(query_hbm, query, local_sem.at[1])
    own_copy = pltpu.make_async_copy(coarse_hbm, coarse.at[row], local_sem.at[2])
    fine_copy.start()
    own_copy.start()
    query_copy.start()

    def each(start, stop, act):
        def body(k, carry):
            act(k)
            return carry

        lax.fori_loop(start, stop, body, 0)

    def ahead(k):
        peer = lax.rem(me + k, team)
        return (peer // half, base + lax.rem(peer, half))

    def behind(k):
        peer = lax.rem(me - k + team, team)
        return (peer // half, base + lax.rem(peer, half))

    opposite = (row, lax.rem(col + half, ncols))
    barrier = pltpu.get_barrier_semaphore()
    pl.semaphore_signal(barrier, inc=1, device_id=opposite, device_id_type=MESH)
    each(
        1,
        team,
        lambda k: pl.semaphore_signal(barrier, inc=1, device_id=ahead(k), device_id_type=MESH),
    )

    super_copy.wait()
    pick_copy.wait()
    ids = chosen_ids[...]
    picks = picked_ids[...]
    candidate = picks >> log2(SBLK)
    parents = jnp.zeros_like(picks)
    for i in range(ids.shape[1]):
        parents = jnp.where(candidate == i, ids[:, i : i + 1], parents)
    fine_ids = (parents << log2(SBLK)) + (picks & (SBLK - 1))
    table[...] = jnp.zeros_like(table)
    table[:blocks, :PICK] = ((fine_ids >> log2(span)) - base + ncols) & (ncols - 1)
    table[blocks : 2 * blocks, :PICK] = fine_ids & (span - 1)
    turned = jnp.transpose(table[...])
    owners = jnp.concatenate([turned[:PICK, b : b + 1] for b in range(blocks)], axis=0)
    local_ids = jnp.concatenate(
        [turned[:PICK, blocks + b : blocks + b + 1] for b in range(blocks)], axis=0
    )
    count = blocks * PICK
    marks = (owners == lax.broadcasted_iota(jnp.int32, (count, LANES), 1)).astype(jnp.float32)
    earlier = lax.broadcasted_iota(jnp.int32, (count, count), 1) < lax.broadcasted_iota(
        jnp.int32, (count, count), 0
    )
    ranks = jnp.dot(
        earlier.astype(jnp.float32).astype(jnp.bfloat16),
        marks.astype(jnp.bfloat16),
        preferred_element_type=jnp.float32,
    )
    slots = jnp.sum(ranks * marks, axis=1, keepdims=True).astype(jnp.int32)
    places = (owners & (half - 1)) * (2 * capacity) + (owners >> log2(half)) * capacity + slots
    matches = places == lax.broadcasted_iota(jnp.int32, (count, ncols * capacity), 1)
    sorter[...] = matches.astype(jnp.float32).astype(jnp.bfloat16)
    outgoing = jnp.sum(jnp.where(matches, local_ids + 1, 0), axis=0, keepdims=True) - 1
    for c in range(half):
        request[c] = jnp.broadcast_to(
            outgoing[:, c * 2 * capacity : (c + 1) * 2 * capacity], (8, 2 * capacity)
        )
    pl.semaphore_wait(barrier, team)

    def ask_copy(k):
        target = ahead(k)
        return pltpu.make_async_remote_copy(
            src_ref=request.at[target[1] - base],
            dst_ref=asked.at[k],
            send_sem=ask_send.at[k],
            recv_sem=ask_recv.at[k],
            device_id=target,
            device_id_type=MESH,
        )

    across_copy = pltpu.make_async_remote_copy(
        src_ref=fine_hbm.at[:, pl.ds(pl.multiple_of(row * part, part), part)],
        dst_ref=across,
        send_sem=across_sem.at[0],
        recv_sem=across_sem.at[1],
        device_id=opposite,
        device_id_type=MESH,
    )

    def near_copy(k):
        return pltpu.make_async_remote_copy(
            src_ref=near_staged.at[k],
            dst_ref=near.at[local],
            send_sem=near_send.at[k],
            recv_sem=near_recv.at[k],
            device_id=(row, base + lax.rem(local - k + half, half)),
            device_id_type=MESH,
        )

    def far_copy(k):
        return pltpu.make_async_remote_copy(
            src_ref=far_staged.at[k],
            dst_ref=far.at[row, local],
            send_sem=far_send.at[k],
            recv_sem=far_recv.at[k],
            device_id=behind(k),
            device_id_type=MESH,
        )

    def coarse_copy(k):
        return pltpu.make_async_remote_copy(
            src_ref=coarse_hbm,
            dst_ref=coarse.at[row],
            send_sem=coarse_send.at[k],
            recv_sem=coarse_recv.at[k],
            device_id=(lax.rem(row + k, nrows), col),
            device_id_type=MESH,
        )

    each(1, team, lambda k: ask_copy(k).start())
    across_copy.start()
    each(1, nrows, lambda k: coarse_copy(k).start())

    asked[0] = request[local]
    row_iota = lax.broadcasted_iota(jnp.int32, (capacity, span), 1)
    fine_copy.wait()
    each(1, team, lambda k: ask_copy(k).wait_recv())

    def one_hot(k, offset):
        ids = jnp.transpose(asked[k])[offset : offset + capacity, 0:1]
        return (ids == row_iota).astype(jnp.float32).astype(jnp.bfloat16)

    def near_group(g, carry):
        picked = []
        for i in range(GROUP):
            other = lax.rem(local - (g * GROUP + i) + half, half)
            picked.append(one_hot(lax.rem(local - other + team, team), 0))
        found = jnp.dot(
            jnp.concatenate(picked, axis=0), fine[...], preferred_element_type=jnp.float32
        ).astype(jnp.bfloat16)
        for i in range(GROUP):
            near_staged[g * GROUP + i] = found[i * capacity : (i + 1) * capacity]
        for i in range(GROUP):
            k = g * GROUP + i

            @pl.when(k > 0)
            def _():
                near_copy(k).start()

        return carry

    lax.fori_loop(0, half // GROUP, near_group, 0)
    near[local] = near_staged[0]
    across_copy.wait_recv()

    def far_group(g, carry):
        picked = [one_hot(g * GROUP + i, capacity) for i in range(GROUP)]
        found = jnp.dot(
            jnp.concatenate(picked, axis=0), across[...], preferred_element_type=jnp.float32
        ).astype(jnp.bfloat16)
        for i in range(GROUP):
            far_staged[g * GROUP + i] = found[i * capacity : (i + 1) * capacity]
        for i in range(GROUP):
            k = g * GROUP + i

            @pl.when(k > 0)
            def _():
                far_copy(k).start()

        return carry

    lax.fori_loop(0, team // GROUP, far_group, 0)
    far[row, local] = far_staged[0]

    query_copy.wait()
    own_copy.wait()
    each(1, nrows, lambda k: coarse_copy(k).wait_recv())

    super_iota = lax.broadcasted_iota(jnp.int32, (supers, PICK), 0)

    def coarse_block(b, carry):
        for h in range(H):
            cut = pl.ds(h * D, D)
            keys = coarse[:, :, cut].reshape(supers, D)
            scores = lax.dot_general(
                query[b, :, cut], keys, (((1,), (1,)), ((), ())), preferred_element_type=jnp.float32
            )
            top = jnp.max(scores, axis=1, keepdims=True)
            raised = jnp.exp2((scores - top) * scale)
            share = 1.0 / jnp.sum(raised, axis=1, keepdims=True)
            portion_ref[b, h : h + 1, :] = jnp.sum(raised * share, axis=0, keepdims=True) * (
                supers / qtok
            )
        return carry

    lax.fori_loop(0, blocks, coarse_block, 0)
    for b in range(blocks):
        weights[b] = jnp.dot(
            portion_ref[b],
            (parents[b : b + 1] == super_iota).astype(jnp.float32),
            preferred_element_type=jnp.float32,
            precision=lax.Precision.HIGHEST,
        )

    cells = ncols * capacity
    each(1, half, lambda k: near_copy(k).wait_recv())
    each(1, team, lambda k: far_copy(k).wait_recv())
    sums = [[] for _ in range(blocks)]
    for q in range(nrows):
        joined = jnp.concatenate([near[:, :, q * part : (q + 1) * part], far[q]], axis=1)
        rows = jnp.dot(
            sorter[...], joined.reshape(cells, part), preferred_element_type=jnp.float32
        )
        rows = rows.astype(jnp.bfloat16)
        for b in range(blocks):
            for i in range(part // D):
                h = q * (part // D) + i
                scores = lax.dot_general(
                    query[b, :, h * D : (h + 1) * D],
                    rows[b * PICK : (b + 1) * PICK, i * D : (i + 1) * D],
                    (((1,), (1,)), ((), ())),
                    preferred_element_type=jnp.float32,
                )
                top = jnp.max(scores, axis=1, keepdims=True)
                raised = jnp.exp2((scores - top) * scale)
                share = 1.0 / jnp.sum(raised, axis=1, keepdims=True)
                sums[b].append(jnp.sum(raised * share, axis=0, keepdims=True))
    for b in range(blocks):
        final = jnp.concatenate(sums[b], axis=0) * weights[b] * (PICK / qtok)
        selected_ref[b : b + 1, :] = jnp.concatenate(
            [final[h : h + 1] for h in range(H)], axis=1
        )

    across_copy.wait_send()
    each(1, team, lambda k: ask_copy(k).wait_send())
    each(1, half, lambda k: near_copy(k).wait_send())
    each(1, team, lambda k: far_copy(k).wait_send())
    each(1, nrows, lambda k: coarse_copy(k).wait_send())


def per_device(queries, coarse_keys, fine_keys, super_ids, picks):
    blocks, qtok, width = queries.shape
    nrows = lax.axis_size("row")
    ncols = lax.axis_size("col")
    half = ncols // 2
    team = nrows * half
    shard = coarse_keys.shape[0]
    supers = shard * nrows
    span = fine_keys.shape[0]
    part = width // nrows
    capacity = blocks // 4 * PICK
    vmem = pl.BlockSpec(memory_space=pltpu.VMEM)
    hbm = pl.BlockSpec(memory_space=pltpu.HBM)
    dma = pltpu.SemaphoreType.DMA
    portion, selected = pl.pallas_call(
        functools.partial(kernel, nrows, ncols, capacity),
        out_shape=(
            jax.ShapeDtypeStruct((blocks, H, supers), jnp.float32),
            jax.ShapeDtypeStruct((blocks, H * PICK), jnp.float32),
        ),
        in_specs=[hbm] * 5,
        out_specs=(vmem, vmem),
        scratch_shapes=[
            pltpu.VMEM((blocks, qtok, width), jnp.bfloat16),
            pltpu.VMEM((span, width), jnp.bfloat16),
            pltpu.VMEM((nrows, shard, width), jnp.bfloat16),
            pltpu.VMEM((span, part), jnp.bfloat16),
            pltpu.VMEM((team, 8, 2 * capacity), jnp.int32),
            pltpu.VMEM((half, capacity, width), jnp.bfloat16),
            pltpu.VMEM((team, capacity, part), jnp.bfloat16),
            pltpu.VMEM((half, capacity, width), jnp.bfloat16),
            pltpu.VMEM((nrows, half, capacity, part), jnp.bfloat16),
            pltpu.VMEM((blocks, H, PICK), jnp.float32),
            pltpu.VMEM(super_ids.shape, jnp.int32),
            pltpu.VMEM(picks.shape, jnp.int32),
            pltpu.VMEM((2 * blocks, LANES), jnp.int32),
            pltpu.VMEM((half, 8, 2 * capacity), jnp.int32),
            pltpu.VMEM((blocks * PICK, ncols * capacity), jnp.bfloat16),
            dma((5,)),
            dma((2,)),
            dma((nrows,)),
            dma((nrows,)),
            dma((team,)),
            dma((team,)),
            dma((half,)),
            dma((half,)),
            dma((team,)),
            dma((team,)),
        ],
        compiler_params=pltpu.CompilerParams(
            collective_id=0, has_side_effects=True, vmem_limit_bytes=63963136
        ),
    )(super_ids, picks, queries, coarse_keys, fine_keys)
    return (portion, selected)


def solution(mesh):
    return jax.shard_map(
        per_device,
        mesh=mesh,
        in_specs=(
            P(("row", "col"), None, None),
            P("row", None),
            P("col", None),
            P(("row", "col"), None),
            P(("row", "col"), None),
        ),
        out_specs=(P(("row", "col"), None, None), P(("row", "col"), None)),
        check_vma=False,
    )
```

```python
import functools
import math

import jax
import jax.numpy as jnp
from jax import lax
from jax.experimental import pallas as pl
from jax.experimental.pallas import tpu as pltpu
from jax.sharding import PartitionSpec as P

H = 8
D = 128
SBLK = 8
PICK = 64
LANES = 128
GROUP = 4
MESH = pl.DeviceIdType.MESH


def log2(value):
    assert value & (value - 1) == 0
    return value.bit_length() - 1


def kernel(
    nrows,
    ncols,
    capacity,
    super_hbm,
    pick_hbm,
    query_hbm,
    coarse_hbm,
    fine_hbm,
    portion_ref,
    selected_ref,
    query,
    fine,
    coarse,
    across,
    asked,
    near_staged,
    far_staged,
    near,
    far,
    weights,
    chosen_ids,
    picked_ids,
    table,
    request,
    sorter,
    local_sem,
    across_sem,
    coarse_send,
    coarse_recv,
    ask_send,
    ask_recv,
    near_send,
    near_recv,
    far_send,
    far_recv,
):
    row = lax.axis_index("row")
    col = lax.axis_index("col")
    half = ncols // 2
    team = nrows * half
    local = lax.rem(col, half)
    base = col - local
    me = row * half + local
    blocks, qtok, width = query.shape
    part = width // nrows
    pieces = part // D
    supers = nrows * coarse.shape[1]
    span = fine.shape[0]
    scale = math.log2(math.e) / math.sqrt(D)

    super_copy = pltpu.make_async_copy(super_hbm, chosen_ids, local_sem.at[3])
    pick_copy = pltpu.make_async_copy(pick_hbm, picked_ids, local_sem.at[4])
    super_copy.start()
    pick_copy.start()
    fine_copy = pltpu.make_async_copy(fine_hbm, fine, local_sem.at[0])
    query_copy = pltpu.make_async_copy(query_hbm, query, local_sem.at[1])
    own_copy = pltpu.make_async_copy(coarse_hbm, coarse.at[row], local_sem.at[2])
    fine_copy.start()
    own_copy.start()
    query_copy.start()

    def each(start, stop, act):
        def body(k, carry):
            act(k)
            return carry

        lax.fori_loop(start, stop, body, 0)

    def ahead(k):
        peer = lax.rem(me + k, team)
        return (peer // half, base + lax.rem(peer, half))

    def behind(k):
        peer = lax.rem(me - k + team, team)
        return (peer // half, base + lax.rem(peer, half))

    opposite = (row, lax.rem(col + half, ncols))
    barrier = pltpu.get_barrier_semaphore()
    pl.semaphore_signal(barrier, inc=1, device_id=opposite, device_id_type=MESH)
    each(
        1,
        team,
        lambda k: pl.semaphore_signal(barrier, inc=1, device_id=ahead(k), device_id_type=MESH),
    )

    super_copy.wait()
    pick_copy.wait()
    ids = chosen_ids[...]
    picks = picked_ids[...]
    candidate = picks >> log2(SBLK)
    parents = jnp.zeros_like(picks)
    for i in range(ids.shape[1]):
        parents = jnp.where(candidate == i, ids[:, i : i + 1], parents)
    fine_ids = (parents << log2(SBLK)) + (picks & (SBLK - 1))
    table[...] = jnp.zeros_like(table)
    table[:blocks, :PICK] = ((fine_ids >> log2(span)) - base + ncols) & (ncols - 1)
    table[blocks : 2 * blocks, :PICK] = fine_ids & (span - 1)
    turned = jnp.transpose(table[...])
    owners = jnp.concatenate([turned[:PICK, b : b + 1] for b in range(blocks)], axis=0)
    local_ids = jnp.concatenate(
        [turned[:PICK, blocks + b : blocks + b + 1] for b in range(blocks)], axis=0
    )
    count = blocks * PICK
    marks = (owners == lax.broadcasted_iota(jnp.int32, (count, LANES), 1)).astype(jnp.float32)
    earlier = lax.broadcasted_iota(jnp.int32, (count, count), 1) < lax.broadcasted_iota(
        jnp.int32, (count, count), 0
    )
    ranks = jnp.dot(
        earlier.astype(jnp.float32).astype(jnp.bfloat16),
        marks.astype(jnp.bfloat16),
        preferred_element_type=jnp.float32,
    )
    slots = jnp.sum(ranks * marks, axis=1, keepdims=True).astype(jnp.int32)
    places = (owners & (half - 1)) * (2 * capacity) + (owners >> log2(half)) * capacity + slots
    matches = places == lax.broadcasted_iota(jnp.int32, (count, ncols * capacity), 1)
    sorter[...] = matches.astype(jnp.float32).astype(jnp.bfloat16)
    outgoing = jnp.sum(jnp.where(matches, local_ids + 1, 0), axis=0, keepdims=True) - 1
    for c in range(half):
        request[c] = jnp.broadcast_to(
            outgoing[:, c * 2 * capacity : (c + 1) * 2 * capacity], (8, 2 * capacity)
        )
    pl.semaphore_wait(barrier, team)

    def ask_copy(k):
        target = ahead(k)
        return pltpu.make_async_remote_copy(
            src_ref=request.at[target[1] - base],
            dst_ref=asked.at[k],
            send_sem=ask_send.at[k],
            recv_sem=ask_recv.at[k],
            device_id=target,
            device_id_type=MESH,
        )

    def across_copy(i):
        return pltpu.make_async_remote_copy(
            src_ref=fine_hbm.at[:, pl.ds(pl.multiple_of(row * part + i * D, D), D)],
            dst_ref=across.at[i],
            send_sem=across_sem.at[i],
            recv_sem=across_sem.at[pieces + i],
            device_id=opposite,
            device_id_type=MESH,
        )

    def near_copy(k):
        return pltpu.make_async_remote_copy(
            src_ref=near_staged.at[k],
            dst_ref=near.at[local],
            send_sem=near_send.at[k],
            recv_sem=near_recv.at[k],
            device_id=(row, base + lax.rem(local - k + half, half)),
            device_id_type=MESH,
        )

    def far_copy(p, k):
        return pltpu.make_async_remote_copy(
            src_ref=far_staged.at[p, k],
            dst_ref=far.at[row, p, local],
            send_sem=far_send.at[p, k],
            recv_sem=far_recv.at[p, k],
            device_id=behind(k),
            device_id_type=MESH,
        )

    def coarse_copy(k):
        return pltpu.make_async_remote_copy(
            src_ref=coarse_hbm,
            dst_ref=coarse.at[row],
            send_sem=coarse_send.at[k],
            recv_sem=coarse_recv.at[k],
            device_id=(lax.rem(row + k, nrows), col),
            device_id_type=MESH,
        )

    each(1, team, lambda k: ask_copy(k).start())
    each(0, pieces, lambda i: across_copy(i).start())
    each(1, nrows, lambda k: coarse_copy(k).start())

    asked[0] = request[local]
    row_iota = lax.broadcasted_iota(jnp.int32, (capacity, span), 1)
    fine_copy.wait()
    each(1, team, lambda k: ask_copy(k).wait_recv())

    def one_hot(k, offset):
        ids = jnp.transpose(asked[k])[offset : offset + capacity, 0:1]
        return (ids == row_iota).astype(jnp.float32).astype(jnp.bfloat16)

    def near_group(g, carry):
        picked = []
        for i in range(GROUP):
            other = lax.rem(local - (g * GROUP + i) + half, half)
            picked.append(one_hot(lax.rem(local - other + team, team), 0))
        found = jnp.dot(
            jnp.concatenate(picked, axis=0), fine[...], preferred_element_type=jnp.float32
        ).astype(jnp.bfloat16)
        for i in range(GROUP):
            near_staged[g * GROUP + i] = found[i * capacity : (i + 1) * capacity]
        for i in range(GROUP):
            k = g * GROUP + i

            @pl.when(k > 0)
            def _():
                near_copy(k).start()

        return carry

    lax.fori_loop(0, half // GROUP, near_group, 0)
    near[local] = near_staged[0]
    def far_group(p, g, carry):
        picked = [one_hot(g * GROUP + i, capacity) for i in range(GROUP)]
        found = jnp.dot(
            jnp.concatenate(picked, axis=0), across[p], preferred_element_type=jnp.float32
        ).astype(jnp.bfloat16)
        for i in range(GROUP):
            far_staged[p, g * GROUP + i] = found[i * capacity : (i + 1) * capacity]
        for i in range(GROUP):
            k = g * GROUP + i

            @pl.when(k > 0)
            def _():
                far_copy(p, k).start()

        return carry

    for p in range(pieces):
        across_copy(p).wait_recv()
        lax.fori_loop(0, team // GROUP, functools.partial(far_group, p), 0)
        far[row, p, local] = far_staged[p, 0]

    query_copy.wait()
    own_copy.wait()
    each(1, nrows, lambda k: coarse_copy(k).wait_recv())

    super_iota = lax.broadcasted_iota(jnp.int32, (supers, PICK), 0)

    def coarse_block(b, carry):
        for h in range(H):
            cut = pl.ds(h * D, D)
            keys = coarse[:, :, cut].reshape(supers, D)
            scores = lax.dot_general(
                query[b, :, cut], keys, (((1,), (1,)), ((), ())), preferred_element_type=jnp.float32
            )
            top = jnp.max(scores, axis=1, keepdims=True)
            raised = jnp.exp2((scores - top) * scale)
            share = 1.0 / jnp.sum(raised, axis=1, keepdims=True)
            portion_ref[b, h : h + 1, :] = jnp.sum(raised * share, axis=0, keepdims=True) * (
                supers / qtok
            )
        return carry

    lax.fori_loop(0, blocks, coarse_block, 0)
    for b in range(blocks):
        weights[b] = jnp.dot(
            portion_ref[b],
            (parents[b : b + 1] == super_iota).astype(jnp.float32),
            preferred_element_type=jnp.float32,
            precision=lax.Precision.HIGHEST,
        )

    cells = ncols * capacity
    each(1, half, lambda k: near_copy(k).wait_recv())
    for p in range(pieces):
        each(1, team, lambda k: far_copy(p, k).wait_recv())
    sums = [[] for _ in range(blocks)]
    for q in range(nrows):
        remote = jnp.concatenate([far[q, p] for p in range(pieces)], axis=2)
        joined = jnp.concatenate([near[:, :, q * part : (q + 1) * part], remote], axis=1)
        rows = jnp.dot(
            sorter[...], joined.reshape(cells, part), preferred_element_type=jnp.float32
        )
        rows = rows.astype(jnp.bfloat16)
        for b in range(blocks):
            for i in range(part // D):
                h = q * (part // D) + i
                scores = lax.dot_general(
                    query[b, :, h * D : (h + 1) * D],
                    rows[b * PICK : (b + 1) * PICK, i * D : (i + 1) * D],
                    (((1,), (1,)), ((), ())),
                    preferred_element_type=jnp.float32,
                )
                top = jnp.max(scores, axis=1, keepdims=True)
                raised = jnp.exp2((scores - top) * scale)
                share = 1.0 / jnp.sum(raised, axis=1, keepdims=True)
                sums[b].append(jnp.sum(raised * share, axis=0, keepdims=True))
    for b in range(blocks):
        final = jnp.concatenate(sums[b], axis=0) * weights[b] * (PICK / qtok)
        selected_ref[b : b + 1, :] = jnp.concatenate(
            [final[h : h + 1] for h in range(H)], axis=1
        )

    each(0, pieces, lambda i: across_copy(i).wait_send())
    each(1, team, lambda k: ask_copy(k).wait_send())
    each(1, half, lambda k: near_copy(k).wait_send())
    for p in range(pieces):
        each(1, team, lambda k: far_copy(p, k).wait_send())
    each(1, nrows, lambda k: coarse_copy(k).wait_send())


def per_device(queries, coarse_keys, fine_keys, super_ids, picks):
    blocks, qtok, width = queries.shape
    nrows = lax.axis_size("row")
    ncols = lax.axis_size("col")
    half = ncols // 2
    team = nrows * half
    shard = coarse_keys.shape[0]
    supers = shard * nrows
    span = fine_keys.shape[0]
    part = width // nrows
    pieces = part // D
    capacity = blocks // 4 * PICK
    vmem = pl.BlockSpec(memory_space=pltpu.VMEM)
    hbm = pl.BlockSpec(memory_space=pltpu.HBM)
    dma = pltpu.SemaphoreType.DMA
    portion, selected = pl.pallas_call(
        functools.partial(kernel, nrows, ncols, capacity),
        out_shape=(
            jax.ShapeDtypeStruct((blocks, H, supers), jnp.float32),
            jax.ShapeDtypeStruct((blocks, H * PICK), jnp.float32),
        ),
        in_specs=[hbm] * 5,
        out_specs=(vmem, vmem),
        scratch_shapes=[
            pltpu.VMEM((blocks, qtok, width), jnp.bfloat16),
            pltpu.VMEM((span, width), jnp.bfloat16),
            pltpu.VMEM((nrows, shard, width), jnp.bfloat16),
            pltpu.VMEM((pieces, span, D), jnp.bfloat16),
            pltpu.VMEM((team, 8, 2 * capacity), jnp.int32),
            pltpu.VMEM((half, capacity, width), jnp.bfloat16),
            pltpu.VMEM((pieces, team, capacity, D), jnp.bfloat16),
            pltpu.VMEM((half, capacity, width), jnp.bfloat16),
            pltpu.VMEM((nrows, pieces, half, capacity, D), jnp.bfloat16),
            pltpu.VMEM((blocks, H, PICK), jnp.float32),
            pltpu.VMEM(super_ids.shape, jnp.int32),
            pltpu.VMEM(picks.shape, jnp.int32),
            pltpu.VMEM((2 * blocks, LANES), jnp.int32),
            pltpu.VMEM((half, 8, 2 * capacity), jnp.int32),
            pltpu.VMEM((blocks * PICK, ncols * capacity), jnp.bfloat16),
            dma((5,)),
            dma((2 * pieces,)),
            dma((nrows,)),
            dma((nrows,)),
            dma((team,)),
            dma((team,)),
            dma((half,)),
            dma((half,)),
            dma((pieces, team)),
            dma((pieces, team)),
        ],
        compiler_params=pltpu.CompilerParams(
            collective_id=0, has_side_effects=True, vmem_limit_bytes=63963136
        ),
    )(super_ids, picks, queries, coarse_keys, fine_keys)
    return (portion, selected)


def solution(mesh):
    return jax.shard_map(
        per_device,
        mesh=mesh,
        in_specs=(
            P(("row", "col"), None, None),
            P("row", None),
            P("col", None),
            P(("row", "col"), None),
            P(("row", "col"), None),
        ),
        out_specs=(P(("row", "col"), None, None), P(("row", "col"), None)),
        check_vma=False,
    )
```
